32 devices in a mesh: gx: 4 (over x, core), gy: 4 (over z), gz: 2 (over y).
Axes of the slice: x: 2, y: 2, z: 4, core: 2. Of those that a mesh axis runs over, the one named last changes fastest.
Arguments:
- fields: float32 [11, 500, 32, 256], P(None, 'gx', 'gy', 'gz'), may hold values from -6 to 6
- var_scale: float32 [11], replicated, may hold values from 0.3 to 3
- start_basis: float32 [500, 64], replicated, may hold values from -6 to 6
Outputs:
- factor: float32 [500, 64], replicated
- core: float32 [64, 11, 32, 256], P('gx', None, 'gy', 'gz')
The draws below stay inside these ranges and needn't reach their ends.
All inputs are finite; a program needn't handle non-finite values.
Results may differ from the reference program's by a relative error of at most 0.0002.
Values sent between devices are 32-bit elements; how exact they have to be, the bound alone decides.
No kernel may reach another device: no remote copies, remote signals or barrier semaphores. Data moves between devices by JAX's collectives and lax.ppermute only.
A program may use at most 128 MiB of HBM per device.

```python
import math
import jax
import jax.numpy as jnp
from jax import lax

V = 11
N1 = 500
RANK = 64
ITERS = 3
N2 = 32
N3 = 256


def steps_of(stream_key, dims, shards, low, largest):
    def one(dim, shards_of):
        heights = jax.random.uniform(jax.random.fold_in(jax.random.fold_in(stream_key, 6), dim), (shards_of,), jnp.float32, low / len(shards), largest / len(shards))
        return jnp.repeat(jnp.exp(heights), dims[dim] // shards_of).reshape((-1,) + (1,) * (len(dims) - dim - 1))

    level = one(*shards[0])
    for cut in shards[1:]:
        level = level * one(*cut)
    return level


def centred(key, shape, width, limit, split=(), dtype=jnp.bfloat16):
    array = jax.random.normal(key, shape, jnp.float32) * width
    if len(split) > 0:
        array = steps_of(key, shape, split, -0.22, 0.18) * array
    return jnp.clip(array, min=-limit, max=limit).astype(dtype)


def setup_inputs(seed: int = 0) -> dict:
    splits = jax.random.split(jax.random.key(seed), 4)
    fields = centred(splits[0], (V, N1, N2, N3), 1.0, 6.0, ((1, 4), (2, 4), (3, 2)), jnp.float32)
    var_scale = jnp.clip(jnp.exp(jax.random.uniform(splits[1], (V,), jnp.float32, math.log(0.3), math.log(3.0))), 0.3, 3.0)
    start_basis = centred(splits[2], (N1, RANK), 1.0, 6.0, (), jnp.float32)
    return dict(fields=fields, var_scale=var_scale, start_basis=start_basis)


def orthonormal(block):
    small = jnp.dot(block.T, block, precision=lax.Precision.HIGHEST)
    lower = jnp.linalg.cholesky(small)
    return jax.scipy.linalg.solve_triangular(lower, block.T, lower=True).T

def reference(fields, var_scale, start_basis):
    scaled = fields * var_scale[:, None, None, None]
    gram = lax.dot_general(scaled, scaled, (((0, 2, 3), (0, 2, 3)), ((), ())), precision=lax.Precision.HIGHEST)
    basis = start_basis
    for step in range(ITERS):
        basis = orthonormal(jnp.dot(gram, basis, precision=lax.Precision.HIGHEST))
    core = lax.dot_general(basis, scaled, (((0,), (1,)), ((), ())), precision=lax.Precision.HIGHEST)
    return (basis, core)
```

```python
import jax
import jax.numpy as jnp
from jax import lax
from jax.sharding import PartitionSpec as P

ITERS = 3
LANE = 128
CHUNKS = 2
HIGH = lax.Precision.HIGH
HIGHEST = lax.Precision.HIGHEST


def swap(array, axis, size, step):
    return lax.ppermute(array, axis, [(i, i ^ step) for i in range(size)])


def orthonormal(block):
    small = jnp.dot(block.T, block, precision=HIGHEST)
    lower = jnp.linalg.cholesky(small)
    return jax.scipy.linalg.solve_triangular(lower, block.T, lower=True).T


def outer(left, right):
    return lax.dot_general(left, right, (((0, 2), (0, 2)), ((), ())), precision=HIGH)


def solution(mesh):
    sizes = dict(mesh.shape)
    nx = sizes["gx"]
    chip = nx // 2

    def sum_columns(part):
        for axis in ("gz", "gy"):
            step = 1
            while step < sizes[axis]:
                part = part + swap(part, axis, sizes[axis], step)
                step *= 2
        return part

    def in_order(mine, me):
        near = swap(mine, "gx", nx, 1)
        far = swap(mine, "gx", nx, chip)
        both = swap(far, "gx", nx, 1)
        stack = jnp.stack([mine, near, far, both])
        return jnp.stack([lax.dynamic_index_in_dim(stack, me ^ g, 0, keepdims=False) for g in range(nx)])

    def per_device(fields, var_scale, start_basis):
        v, rows, j, k = fields.shape
        rank = start_basis.shape[1]
        keep = rank // nx
        pad = -(-rows // LANE) * LANE
        me = lax.axis_index("gx")
        x = me // chip
        scaled = fields * var_scale[:, None, None, None]
        tall = jnp.pad(scaled.transpose(2, 0, 1, 3), ((0, 0), (0, 0), (0, pad - rows), (0, 0)))
        half = j // 2

        def half_of(array, which):
            return lax.dynamic_slice_in_dim(array, which * half, half, 0).reshape(half * v, -1, k)

        ours = half_of(tall, x)
        theirs = half_of(tall, 1 - x)
        cut = pad // CHUNKS
        far = [swap(theirs[:, q * cut:(q + 1) * cut], "gx", nx, chip) for q in range(CHUNKS)]
        near = swap(tall, "gx", nx, 1)
        whole = tall.reshape(j * v, pad, k)
        diag = sum_columns(jnp.stack([outer(whole, whole), outer(near.reshape(j * v, pad, k), whole)]))
        near_half = half_of(near, x)
        cross = [sum_columns(jnp.stack([outer(ours, f), outer(near_half, f)])) for f in far]
        cross = jnp.concatenate(cross, axis=2)
        diag, cross = in_order(diag, me), in_order(cross, me)
        rows_of = []
        for b in range(nx):
            blocks = [None] * nx
            blocks[b] = diag[b, 0]
            blocks[b ^ 1] = diag[b ^ 1, 1]
            blocks[b ^ chip] = cross[b, 0] + cross[b ^ chip, 0].T
            blocks[b ^ chip ^ 1] = cross[b ^ 1, 1] + cross[b ^ chip, 1].T
            rows_of.append(jnp.concatenate(blocks, axis=1))
        gram = jnp.concatenate(rows_of, axis=0)
        basis = jnp.pad(start_basis.reshape(nx, rows, rank), ((0, 0), (0, pad - rows), (0, 0))).reshape(nx * pad, rank)
        for step in range(ITERS):
            basis = orthonormal(jnp.dot(gram, basis, precision=HIGHEST))
        basis = basis.reshape(nx, pad, rank)
        far = jnp.concatenate(far, axis=1)
        both = swap(far, "gx", nx, 1)
        held = [ours, near_half, far, both]

        def ranks(which):
            out = 0.0
            for s, data in enumerate((0, 1, chip, chip ^ 1)):
                own = lax.dynamic_index_in_dim(basis, me ^ data, 0, keepdims=False)
                own = lax.dynamic_slice_in_dim(own, which * keep, keep, 1)
                out = out + lax.dot_general(own, held[s], (((0,), (1,)), ((), ())), precision=HIGH)
            return out

        got = swap(ranks(me ^ chip), "gx", nx, chip)
        kept = ranks(me)
        low = jnp.where(x == 0, kept, got)
        high = jnp.where(x == 0, got, kept)
        core = jnp.concatenate([low, high], axis=1).reshape(keep, j, v, k).transpose(0, 2, 1, 3)
        return basis[:, :rows].reshape(nx * rows, rank), core

    in_specs = (P(None, "gx", "gy", "gz"), P(), P())
    out_specs = (P(), P("gx", None, "gy", "gz"))
    return jax.shard_map(per_device, mesh=mesh, in_specs=in_specs, out_specs=out_specs, check_vma=False)
```

```python
import jax
import jax.numpy as jnp
from jax import lax
from jax.experimental import pallas as pl
from jax.experimental.pallas import tpu as pltpu
from jax.sharding import PartitionSpec as P


ITERS = 3
LANE = 128
SUB = 8
V_EARLY = 4
V_LATE = 8
TAIL = 4
RATE = 1e9
PACK_MIB = (59, 50)
DIAG_MIB = 8
CROSS_MIB = 8
SOLVE_MIB = 16
HIGHEST = lax.Precision.HIGHEST
F32 = jnp.float32
BF16 = jnp.bfloat16
NT = (((1,), (1,)), ((), ()))
NN = (((1,), (0,)), ((), ()))


def split(x):
    high = x.astype(BF16)
    return high, (x - high.astype(F32)).astype(BF16)


def mm(a, b, dims):
    return lax.dot_general(a, b, dims, preferred_element_type=F32)


def vmem():
    return pl.BlockSpec(memory_space=pltpu.VMEM)


def smem():
    return pl.BlockSpec(memory_space=pltpu.SMEM)


def fill(out, spot, buf, a, scale, first, step, count, half, width):
    tail = count // SUB * SUB
    for j in range(half):
        lanes = slice((spot * half + j) * width, (spot * half + j + 1) * width)
        if tail < out.shape[0]:
            out[tail:, lanes] = jnp.zeros((out.shape[0] - tail, width), F32)
        out[:count, lanes] = buf[a, pl.ds(first + j, count, stride=step), :] * scale


def limit(mib):
    return pltpu.CompilerParams(vmem_limit_bytes=mib * 1024 * 1024)


def cost(micros):
    return pl.CostEstimate(flops=int(micros * RATE), bytes_accessed=0, transcendentals=0)


def pack(fields, scale, x, rows, pad, j, whole):
    v, _, width = fields.shape
    half, cut = j // 2, pad - pad // TAIL
    early = V_EARLY
    count = v if whole else early

    def body(x_ref, s_ref, f_ref, *refs):
        *outs, buf, sems = refs
        span = rows if whole else cut
        copies = [
            pltpu.make_async_copy(f_ref.at[a, pl.ds(0, span * j)], buf.at[a], sems.at[a]) for a in range(count)
        ]
        for copy in copies:
            copy.start()
        other = (1 - x_ref[0]) * half
        for a in range(count):
            copies[a].wait()
            if not whole:
                fill(outs[0], a, buf, a, s_ref[a], other, j, cut, half, width)
                continue
            late, low, high, ours = outs
            if a >= early:
                fill(late, a - early, buf, a, s_ref[a], other, j, cut, half, width)
            piece, b = (low, a) if a < V_LATE else (high, a - V_LATE)
            fill(piece, b, buf, a, s_ref[a], cut * j + other, j, rows - cut, half, width)
            fill(ours, a, buf, a, s_ref[a], x_ref[0] * half, j, rows, half, width)

    def shape(n, height):
        return jax.ShapeDtypeStruct((height, n * half * width), F32)

    shapes = [shape(early, cut)]
    if whole:
        shapes = [shape(v - early, cut), shape(V_LATE, pad - cut), shape(v - V_LATE, pad - cut), shape(v, pad)]
    return pl.pallas_call(
        body,
        out_shape=shapes,
        in_specs=[smem(), smem(), pl.BlockSpec(memory_space=pltpu.HBM)],
        out_specs=[vmem()] * len(shapes),
        scratch_shapes=[
            pltpu.VMEM((count, (rows if whole else cut) * j, width), F32),
            pltpu.SemaphoreType.DMA((count,)),
        ],
        cost_estimate=cost(5 if whole else 2),
        compiler_params=limit(PACK_MIB[whole]),
        name="pack_rest" if whole else "pack_first",
    )(x, scale, fields)


def diagonal(ours, theirs, near_ours, near_theirs, v):
    pad, total = ours.shape
    width = total // v

    def body(o_ref, a1, a2, b1, b2, n_ref, c1, c2, d1, d2, high, low, diag):
        diag[...] = jnp.zeros_like(diag)

        def at(a):
            return pl.ds(pl.multiple_of(a * width, width), width)

        def add(own, near):
            own, near = split(own), split(near)
            chip_high = jnp.concatenate([own[0], near[0]], 0)
            chip_low = jnp.concatenate([own[1], near[1]], 0)
            high_t, low_t = chip_high.T, chip_low.T
            both = mm(jnp.concatenate(own, 0), high_t, NN)
            diag[...] += both[:pad] + both[pad:] + mm(own[0], low_t, NN)
            return chip_high, chip_low

        def mine(a, carry):
            lanes = at(a)
            high[:, lanes], low[:, lanes] = add(o_ref[:, lanes], n_ref[:, lanes])
            return carry

        lax.fori_loop(0, v, mine, 0)
        for first, last in segments(v):
            p = (a1, c1, 0) if first < V_EARLY else (a2, c2, V_EARLY)
            q = (b1, d1, 0) if first < V_LATE else (b2, d2, V_LATE)

            def other(a, carry, p=p, q=q):
                top, bottom = at(a - p[2]), at(a - q[2])
                own = jnp.concatenate([p[0][:, top], q[0][:, bottom]], 0)
                add(own, jnp.concatenate([p[1][:, top], q[1][:, bottom]], 0))
                return carry

            lax.fori_loop(first, last, other, 0)

    half = jax.ShapeDtypeStruct((2 * pad, total), BF16)
    return pl.pallas_call(
        body,
        out_shape=(half, half, jax.ShapeDtypeStruct((pad, 2 * pad), F32)),
        in_specs=[vmem()] * 10,
        out_specs=(vmem(),) * 3,
        cost_estimate=cost(12),
        compiler_params=limit(DIAG_MIB),
        name="diagonal",
    )(ours, *theirs, near_ours, *near_theirs)


def segments(v):
    edges = sorted({0, V_EARLY, V_LATE, v})
    return list(zip(edges[:-1], edges[1:]))


def crossing(high, low, pieces, base, first):
    cut = pieces[0].shape[0]
    pad = high.shape[0] // 2

    def body(h_ref, l_ref, *refs):
        out = refs[-1]
        spot = first
        total = 0.0
        for ref in refs[:len(pieces)]:
            lanes = slice(spot, spot + ref.shape[1])
            top, bottom = split(ref[...].T)
            both = mm(h_ref[:, lanes], jnp.concatenate([top, bottom], 1), NN)
            total = total + both[:, :cut] + both[:, cut:] + mm(l_ref[:, lanes], top, NN)
            spot += ref.shape[1]
        total = total.T
        out[...] = total if base is None else refs[-2][...] + total

    extra = [] if base is None else [base]
    return pl.pallas_call(
        body,
        out_shape=jax.ShapeDtypeStruct((cut, 2 * pad), F32),
        in_specs=[vmem()] * (2 + len(pieces) + len(extra)),
        out_specs=vmem(),
        cost_estimate=cost(3),
        compiler_params=limit(CROSS_MIB),
        name="crossing",
    )(high, low, *pieces, *extra)


def inverse_factor(work, out, rank):
    for p in range(rank // SUB):
        top = p * SUB
        lane = rank + top
        groups = range(p + 1, rank // SUB)
        cols = {}
        for g in groups:
            tile = work[g * SUB:(g + 1) * SUB, :]
            for k in range(SUB):
                cols[g, k] = jnp.broadcast_to(tile[:, lane + k:lane + k + 1], (SUB, 2 * rank))
        rows = [work[pl.ds(top + k, SUB, stride=0), :] for k in range(SUB)]
        small = {}
        for a in range(SUB):
            for b in range(a + 1):
                small[a, b] = jnp.broadcast_to(rows[a][:, lane + b:lane + b + 1], (SUB, 2 * rank))
        for k in range(SUB):
            pivot = small[k, k]
            inv = 1.0 / pivot
            out[top + k:top + k + 1, :] = (rows[k] * lax.rsqrt(pivot))[:1]
            scaled = rows[k] * inv
            for a in range(k + 1, SUB):
                low = small[a, k]
                rows[a] = rows[a] - low * scaled
                low = low * inv
                for b in range(k + 1, a + 1):
                    small[a, b] = small[a, b] - low * small[b, k]
                for g in groups:
                    cols[g, a] = cols[g, a] - cols[g, k] * low
            rows[k] = scaled
        for g in groups:
            tile = work[g * SUB:(g + 1) * SUB, :]
            for k in range(SUB):
                tile = tile - cols[g, k] * rows[k]
            work[g * SUB:(g + 1) * SUB, :] = tile


def solve(me, start, diags, crosses, high, low, far, both, nx, v):
    rank = start.shape[0]
    pad = diags[0].shape[0]
    cuts = len(crosses)
    tops = [0, crosses[0][0].shape[0]]
    total = high.shape[1]
    width = total // v
    chip = nx // 2
    keep = rank // nx
    order = (0, 1, chip, chip ^ 1)

    def assemble(me_ref, d_in, c_in, gram, diag, cross):
        for s in range(nx):
            spot = me_ref[0] ^ order[s]
            diag[spot] = d_in[s][...]
            for q in range(cuts):
                cross[spot, tops[q]:tops[q] + c_in[q][s].shape[0], :] = c_in[q][s][...]
        for b in range(nx):
            at = slice(b * pad, (b + 1) * pad)
            for other, block in (
                (b, diag[b, :, :pad]),
                (b ^ 1, diag[b, :, pad:]),
                (b ^ chip, cross[b ^ chip, :, :pad] + cross[b, :, :pad].T),
                (b ^ chip ^ 1, cross[b ^ chip, :, pad:] + cross[b ^ 1, :, pad:].T),
            ):
                gram[at, other * pad:(other + 1) * pad] = block

    def iterate(s_ref, gram, work, inv, basis):
        eye_rows = lax.broadcasted_iota(jnp.int32, (rank, 2 * rank), 0)
        eye_cols = lax.broadcasted_iota(jnp.int32, (rank, 2 * rank), 1)
        eye = jnp.where(eye_rows == eye_cols, 1.0, 0.0).astype(F32)
        now = s_ref[...]
        for _ in range(ITERS):
            block = lax.dot_general(now, gram[...], NN, precision=HIGHEST, preferred_element_type=F32)
            twice = jnp.concatenate([jnp.zeros_like(block), block], 0)
            work[...] = eye + lax.dot_general(block, twice, NT, precision=HIGHEST, preferred_element_type=F32)
            inverse_factor(work, inv, rank)
            now = lax.dot_general(inv[:, :rank], block, NN, precision=HIGHEST, preferred_element_type=F32)
        for b in range(nx):
            basis[b] = now[:, b * pad:(b + 1) * pad]

    def body(me_ref, s_ref, *refs):
        d_in = refs[:nx]
        c_in = [refs[nx * (q + 1):nx * (q + 2)] for q in range(cuts)]
        refs = refs[nx * (1 + cuts):]
        h_ref, l_ref = refs[:2]
        pieces = refs[2:10]
        basis, kept, sent, gram, diag, cross, work, inv, tail_high, tail_low = refs[10:]
        for q in range(4):
            rows = slice(q // 2 * pad + tops[q % 2], q // 2 * pad + tops[q % 2] + pieces[2 * q].shape[0])
            lanes = [slice(0, pieces[2 * q].shape[1]), slice(pieces[2 * q].shape[1], total)]
            for piece, at in zip(pieces[2 * q:2 * q + 2], lanes):
                tail_high[rows, at], tail_low[rows, at] = split(piece[...])
        assemble(me_ref, d_in, c_in, gram, diag, cross)
        iterate(s_ref, gram, work, inv, basis)
        here = me_ref[0]
        parts = []
        for s in order:
            block = basis.at[here ^ s]
            ranks = [block[pl.ds(pl.multiple_of((here ^ r) * keep, keep), keep), :] for r in (0, chip)]
            parts.append(jnp.concatenate(ranks, 0))
        left = jnp.concatenate(split(jnp.concatenate(parts, 1)), 0)
        near, away = left[:, :2 * pad], left[:, 2 * pad:]
        for a in range(v):
            at = slice(a * width, (a + 1) * width)
            out = mm(near, h_ref[:, at], NN) + mm(away, tail_high[:, at], NN)
            out = out[:2 * keep] + out[2 * keep:]
            out = out + mm(near[:2 * keep], l_ref[:, at], NN) + mm(away[:2 * keep], tail_low[:, at], NN)
            kept[a] = out[:keep]
            sent[a] = out[keep:]

    shape = jax.ShapeDtypeStruct((v, keep, width), F32)
    return pl.pallas_call(
        body,
        out_shape=(jax.ShapeDtypeStruct((nx, rank, pad), F32), shape, shape),
        in_specs=[smem()] + [vmem()] * (1 + nx * (1 + cuts) + 10),
        out_specs=(vmem(), vmem(), vmem()),
        scratch_shapes=[
            pltpu.VMEM((nx * pad, nx * pad), F32),
            pltpu.VMEM((nx, pad, 2 * pad), F32),
            pltpu.VMEM((nx, pad, 2 * pad), F32),
            pltpu.VMEM((rank, 2 * rank), F32),
            pltpu.VMEM((rank, 2 * rank), F32),
            pltpu.VMEM((2 * pad, total), BF16),
            pltpu.VMEM((2 * pad, total), BF16),
        ],
        cost_estimate=cost(15),
        compiler_params=limit(SOLVE_MIB),
        name="solve",
    )(me, start, *diags, *[c for group in crosses for c in group], high, low, *far, *both)


def place(x, kept, got, j):
    v, keep, width = kept.shape
    half = j // 2
    k = width // half

    def body(x_ref, a_ref, b_ref, out):
        for data, first in ((a_ref, x_ref[0] * half), (b_ref, (1 - x_ref[0]) * half)):
            for a in range(v):
                for i in range(half):
                    out[pl.ds(a * j + first + i, keep, stride=v * j), :] = data[a, :, i * k:(i + 1) * k]

    return pl.pallas_call(
        body,
        out_shape=jax.ShapeDtypeStruct((keep * v * j, k), F32),
        in_specs=[smem(), vmem(), vmem()],
        out_specs=vmem(),
        cost_estimate=cost(2),
        compiler_params=limit(8),
        name="place",
    )(x, kept, got).reshape(keep, v, j, k)


def solution(mesh):
    sizes = dict(mesh.shape)
    nx = sizes["gx"]
    chip = nx // 2

    def swap(array, step, axis="gx"):
        return lax.ppermute(array, axis, [(i, i ^ step) for i in range(sizes[axis])])

    def sum_columns(part):
        for axis in ("gz", "gy"):
            step = 1
            while step < sizes[axis]:
                part = part + swap(part, step, axis)
                step *= 2
        return part

    def everywhere(mine):
        far = swap(mine, chip)
        return [mine, swap(mine, 1), far, swap(far, 1)]

    def program(fields, var_scale, start_basis):
        v, rows, j, k = fields.shape
        rank = start_basis.shape[1]
        pad = -(-rows // LANE) * LANE
        me = lax.axis_index("gx").reshape(1)
        x = me // chip
        flat = fields.reshape(v, rows * j, k)
        (first,) = pack(flat, var_scale, x, rows, pad, j, False)
        *rest, ours = pack(flat, var_scale, x, rows, pad, j, True)
        theirs = [first, *rest]
        far = []
        for t in theirs:
            far.append(swap(t, chip))
        near_ours = swap(ours, 1)
        near_theirs = [swap(t, 1) for t in theirs]
        high, low, diag = diagonal(ours, theirs, near_ours, near_theirs, v)
        diag = sum_columns(diag)
        diags = everywhere(diag)
        top = crossing(high, low, far[:2], None, 0)
        top = sum_columns(top)
        bottom = crossing(high, low, far[2:3], None, 0)
        bottom = crossing(high, low, far[3:], bottom, far[2].shape[1])
        crosses = [everywhere(top), everywhere(sum_columns(bottom))]
        both = [swap(f, 1) for f in far]
        start = start_basis.T.reshape(rank, nx, rows)
        start = jnp.pad(start, ((0, 0), (0, 0), (0, pad - rows))).reshape(rank, nx * pad)
        basis, kept, sent = solve(me, start, diags, crosses, high, low, far, both, nx, v)
        core = place(x, kept, swap(sent, chip), j)
        factor = basis[:, :, :rows].transpose(1, 0, 2).reshape(rank, nx * rows).T
        return factor, core

    in_specs = (P(None, "gx", "gy", "gz"), P(), P())
    out_specs = (P(), P("gx", None, "gy", "gz"))
    return jax.shard_map(program, mesh=mesh, in_specs=in_specs, out_specs=out_specs, check_vma=False)
```

```python
import jax
import jax.numpy as jnp
from jax import lax
from jax.experimental import pallas as pl
from jax.experimental.pallas import tpu as pltpu
from jax.sharding import PartitionSpec as P


ITERS = 3
LANE = 128
SUB = 8
V_EARLY = 2
V_LATE = 8
TAIL = 4
RATE = 1e9
PACK_MIB = (59, 50)
DIAG_MIB = 8
CROSS_MIB = 8
SOLVE_MIB = 16
HIGHEST = lax.Precision.HIGHEST
F32 = jnp.float32
BF16 = jnp.bfloat16
NT = (((1,), (1,)), ((), ()))
NN = (((1,), (0,)), ((), ()))


def split(x):
    high = x.astype(BF16)
    return high, (x - high.astype(F32)).astype(BF16)


def mm(a, b, dims):
    return lax.dot_general(a, b, dims, preferred_element_type=F32)


def vmem():
    return pl.BlockSpec(memory_space=pltpu.VMEM)


def smem():
    return pl.BlockSpec(memory_space=pltpu.SMEM)


def fill(out, spot, buf, a, scale, first, step, count, half, width):
    tail = count // SUB * SUB
    for j in range(half):
        lanes = slice((spot * half + j) * width, (spot * half + j + 1) * width)
        if tail < out.shape[0]:
            out[tail:, lanes] = jnp.zeros((out.shape[0] - tail, width), F32)
        out[:count, lanes] = buf[a, pl.ds(first + j, count, stride=step), :] * scale


def limit(mib):
    return pltpu.CompilerParams(vmem_limit_bytes=mib * 1024 * 1024)


def cost(micros):
    return pl.CostEstimate(flops=int(micros * RATE), bytes_accessed=0, transcendentals=0)


def pack(fields, scale, x, rows, pad, j, whole):
    v, _, width = fields.shape
    half, cut = j // 2, pad - pad // TAIL
    early = V_EARLY
    count = v if whole else early

    def body(x_ref, s_ref, f_ref, *refs):
        *outs, buf, sems = refs
        span = rows if whole else cut
        copies = [
            pltpu.make_async_copy(f_ref.at[a, pl.ds(0, span * j)], buf.at[a], sems.at[a]) for a in range(count)
        ]
        for copy in copies:
            copy.start()
        other = (1 - x_ref[0]) * half
        for a in range(count):
            copies[a].wait()
            if not whole:
                fill(outs[0], a, buf, a, s_ref[a], other, j, cut, half, width)
                continue
            late, low, high, ours = outs
            if a >= early:
                fill(late, a - early, buf, a, s_ref[a], other, j, cut, half, width)
            piece, b = (low, a) if a < V_LATE else (high, a - V_LATE)
            fill(piece, b, buf, a, s_ref[a], cut * j + other, j, rows - cut, half, width)
            fill(ours, a, buf, a, s_ref[a], x_ref[0] * half, j, rows, half, width)

    def shape(n, height):
        return jax.ShapeDtypeStruct((height, n * half * width), F32)

    shapes = [shape(early, cut)]
    if whole:
        shapes = [shape(v - early, cut), shape(V_LATE, pad - cut), shape(v - V_LATE, pad - cut), shape(v, pad)]
    return pl.pallas_call(
        body,
        out_shape=shapes,
        in_specs=[smem(), smem(), pl.BlockSpec(memory_space=pltpu.HBM)],
        out_specs=[vmem()] * len(shapes),
        scratch_shapes=[
            pltpu.VMEM((count, (rows if whole else cut) * j, width), F32),
            pltpu.SemaphoreType.DMA((count,)),
        ],
        cost_estimate=cost(5 if whole else 2),
        compiler_params=limit(PACK_MIB[whole]),
        name="pack_rest" if whole else "pack_first",
    )(x, scale, fields)


def diagonal(ours, theirs, near_ours, near_theirs, v):
    pad, total = ours.shape
    width = total // v

    def body(o_ref, a1, a2, b1, b2, n_ref, c1, c2, d1, d2, high, low, tall_high, tall_low, diag):
        diag[...] = jnp.zeros_like(diag)

        def at(a):
            return pl.ds(pl.multiple_of(a * width, width), width)

        def add(own, near):
            own, near = split(own), split(near)
            chip_high = jnp.concatenate([own[0], near[0]], 0)
            chip_low = jnp.concatenate([own[1], near[1]], 0)
            high_t, low_t = chip_high.T, chip_low.T
            both = mm(jnp.concatenate(own, 0), high_t, NN)
            diag[...] += both[:pad] + both[pad:] + mm(own[0], low_t, NN)
            return chip_high, chip_low, high_t, low_t

        def mine(a, carry):
            lanes = at(a)
            high[:, lanes], low[:, lanes], tall_high[lanes, :], tall_low[lanes, :] = add(o_ref[:, lanes], n_ref[:, lanes])
            return carry

        lax.fori_loop(0, v, mine, 0)
        for first, last in segments(v):
            p = (a1, c1, 0) if first < V_EARLY else (a2, c2, V_EARLY)
            q = (b1, d1, 0) if first < V_LATE else (b2, d2, V_LATE)

            def other(a, carry, p=p, q=q):
                top, bottom = at(a - p[2]), at(a - q[2])
                own = jnp.concatenate([p[0][:, top], q[0][:, bottom]], 0)
                add(own, jnp.concatenate([p[1][:, top], q[1][:, bottom]], 0))
                return carry

            lax.fori_loop(first, last, other, 0)

    half = jax.ShapeDtypeStruct((2 * pad, total), BF16)
    tall = jax.ShapeDtypeStruct((total, 2 * pad), BF16)
    return pl.pallas_call(
        body,
        out_shape=(half, half, tall, tall, jax.ShapeDtypeStruct((pad, 2 * pad), F32)),
        in_specs=[vmem()] * 10,
        out_specs=(vmem(),) * 5,
        cost_estimate=cost(12),
        compiler_params=limit(DIAG_MIB),
        name="diagonal",
    )(ours, *theirs, near_ours, *near_theirs)


def segments(v):
    edges = sorted({0, V_EARLY, V_LATE, v})
    return list(zip(edges[:-1], edges[1:]))


def crossing(tall_high, tall_low, pieces, base, first):
    cut = pieces[0].shape[0]
    pad = tall_high.shape[1] // 2

    def body(h_ref, l_ref, *refs):
        out = refs[-1]
        spot = first
        total = refs[-2][...] if base is not None else 0.0
        for ref in refs[:len(pieces)]:
            top, bottom = split(ref[...])
            rows = slice(spot, spot + ref.shape[1])
            both = mm(jnp.concatenate([top, bottom], 0), h_ref[rows, :], NN)
            total = total + both[:cut] + both[cut:] + mm(top, l_ref[rows, :], NN)
            spot += ref.shape[1]
        out[...] = total

    extra = [] if base is None else [base]
    return pl.pallas_call(
        body,
        out_shape=jax.ShapeDtypeStruct((cut, 2 * pad), F32),
        in_specs=[vmem()] * (2 + len(pieces) + len(extra)),
        out_specs=vmem(),
        cost_estimate=cost(3),
        compiler_params=limit(CROSS_MIB),
        name="crossing",
    )(tall_high, tall_low, *pieces, *extra)


def add(one, two, keep):
    def body(a_ref, b_ref, *refs):
        refs[-1][...] = a_ref[...] + b_ref[...]

    return pl.pallas_call(
        body,
        out_shape=jax.ShapeDtypeStruct(one.shape, F32),
        in_specs=[vmem()] * (2 + len(keep)),
        out_specs=vmem(),
        cost_estimate=cost(0.5),
        compiler_params=limit(4),
        name="add",
    )(one, two, *keep)


def inverse_factor(work, out, rank):
    for p in range(rank // SUB):
        top = p * SUB
        lane = rank + top
        groups = range(p + 1, rank // SUB)
        cols = {}
        for g in groups:
            tile = work[g * SUB:(g + 1) * SUB, :]
            for k in range(SUB):
                cols[g, k] = jnp.broadcast_to(tile[:, lane + k:lane + k + 1], (SUB, 2 * rank))
        rows = [work[pl.ds(top + k, SUB, stride=0), :] for k in range(SUB)]
        small = {}
        for a in range(SUB):
            for b in range(a + 1):
                small[a, b] = jnp.broadcast_to(rows[a][:, lane + b:lane + b + 1], (SUB, 2 * rank))
        for k in range(SUB):
            pivot = small[k, k]
            inv = 1.0 / pivot
            out[top + k:top + k + 1, :] = (rows[k] * lax.rsqrt(pivot))[:1]
            scaled = rows[k] * inv
            for a in range(k + 1, SUB):
                low = small[a, k]
                rows[a] = rows[a] - low * scaled
                low = low * inv
                for b in range(k + 1, a + 1):
                    small[a, b] = small[a, b] - low * small[b, k]
                for g in groups:
                    cols[g, a] = cols[g, a] - cols[g, k] * low
            rows[k] = scaled
        for g in groups:
            tile = work[g * SUB:(g + 1) * SUB, :]
            for k in range(SUB):
                tile = tile - cols[g, k] * rows[k]
            work[g * SUB:(g + 1) * SUB, :] = tile


def solve(me, start, diags, crosses, high, low, far, both, nx, v):
    rank = start.shape[0]
    pad = diags[0].shape[0]
    cuts = len(crosses)
    tops = [0, crosses[0][0].shape[0]]
    total = high.shape[1]
    width = total // v
    chip = nx // 2
    keep = rank // nx
    order = (0, 1, chip, chip ^ 1)

    def assemble(me_ref, d_in, c_in, gram, diag, cross):
        for s in range(nx):
            spot = me_ref[0] ^ order[s]
            diag[spot] = d_in[s][...]
            for q in range(cuts):
                cross[spot, tops[q]:tops[q] + c_in[q][s].shape[0], :] = c_in[q][s][...]
        for b in range(nx):
            at = slice(b * pad, (b + 1) * pad)
            for other, block in (
                (b, diag[b, :, :pad]),
                (b ^ 1, diag[b, :, pad:]),
                (b ^ chip, cross[b ^ chip, :, :pad] + cross[b, :, :pad].T),
                (b ^ chip ^ 1, cross[b ^ chip, :, pad:] + cross[b ^ 1, :, pad:].T),
            ):
                gram[at, other * pad:(other + 1) * pad] = block

    def iterate(s_ref, gram, work, inv, basis):
        eye_rows = lax.broadcasted_iota(jnp.int32, (rank, 2 * rank), 0)
        eye_cols = lax.broadcasted_iota(jnp.int32, (rank, 2 * rank), 1)
        eye = jnp.where(eye_rows == eye_cols, 1.0, 0.0).astype(F32)
        now = s_ref[...]
        gram_high, gram_low = split(gram[...])
        for _ in range(ITERS):
            both = mm(jnp.concatenate(split(now), 0), gram_high, NN)
            block = both[:rank] + both[rank:] + mm(now.astype(BF16), gram_low, NN)
            twice = jnp.concatenate([jnp.zeros_like(block), block], 0)
            work[...] = eye + lax.dot_general(block, twice, NT, precision=HIGHEST, preferred_element_type=F32)
            inverse_factor(work, inv, rank)
            now = lax.dot_general(inv[:, :rank], block, NN, precision=HIGHEST, preferred_element_type=F32)
        for b in range(nx):
            basis[b] = now[:, b * pad:(b + 1) * pad]

    def body(me_ref, s_ref, *refs):
        d_in = refs[:nx]
        c_in = [refs[nx * (q + 1):nx * (q + 2)] for q in range(cuts)]
        refs = refs[nx * (1 + cuts):]
        h_ref, l_ref = refs[:2]
        pieces = refs[2:10]
        basis, kept, sent, gram, diag, cross, work, inv, tail_high, tail_low = refs[10:]
        for q in range(4):
            rows = slice(q // 2 * pad + tops[q % 2], q // 2 * pad + tops[q % 2] + pieces[2 * q].shape[0])
            lanes = [slice(0, pieces[2 * q].shape[1]), slice(pieces[2 * q].shape[1], total)]
            for piece, at in zip(pieces[2 * q:2 * q + 2], lanes):
                tail_high[rows, at], tail_low[rows, at] = split(piece[...])
        assemble(me_ref, d_in, c_in, gram, diag, cross)
        iterate(s_ref, gram, work, inv, basis)
        here = me_ref[0]
        parts = []
        for s in order:
            block = basis.at[here ^ s]
            ranks = [block[pl.ds(pl.multiple_of((here ^ r) * keep, keep), keep), :] for r in (0, chip)]
            parts.append(jnp.concatenate(ranks, 0))
        left = jnp.concatenate(split(jnp.concatenate(parts, 1)), 0)
        near, away = left[:, :2 * pad], left[:, 2 * pad:]
        for a in range(v):
            at = slice(a * width, (a + 1) * width)
            out = mm(near, h_ref[:, at], NN) + mm(away, tail_high[:, at], NN)
            out = out[:2 * keep] + out[2 * keep:]
            out = out + mm(near[:2 * keep], l_ref[:, at], NN) + mm(away[:2 * keep], tail_low[:, at], NN)
            kept[a] = out[:keep]
            sent[a] = out[keep:]

    shape = jax.ShapeDtypeStruct((v, keep, width), F32)
    return pl.pallas_call(
        body,
        out_shape=(jax.ShapeDtypeStruct((nx, rank, pad), F32), shape, shape),
        in_specs=[smem()] + [vmem()] * (1 + nx * (1 + cuts) + 10),
        out_specs=(vmem(), vmem(), vmem()),
        scratch_shapes=[
            pltpu.VMEM((nx * pad, nx * pad), F32),
            pltpu.VMEM((nx, pad, 2 * pad), F32),
            pltpu.VMEM((nx, pad, 2 * pad), F32),
            pltpu.VMEM((rank, 2 * rank), F32),
            pltpu.VMEM((rank, 2 * rank), F32),
            pltpu.VMEM((2 * pad, total), BF16),
            pltpu.VMEM((2 * pad, total), BF16),
        ],
        cost_estimate=cost(15),
        compiler_params=limit(SOLVE_MIB),
        name="solve",
    )(me, start, *diags, *[c for group in crosses for c in group], high, low, *far, *both)


def place(x, kept, got, j):
    v, keep, width = kept.shape
    half = j // 2
    k = width // half

    def body(x_ref, a_ref, b_ref, out):
        for data, first in ((a_ref, x_ref[0] * half), (b_ref, (1 - x_ref[0]) * half)):
            for a in range(v):
                for i in range(half):
                    out[pl.ds(a * j + first + i, keep, stride=v * j), :] = data[a, :, i * k:(i + 1) * k]

    return pl.pallas_call(
        body,
        out_shape=jax.ShapeDtypeStruct((keep * v * j, k), F32),
        in_specs=[smem(), vmem(), vmem()],
        out_specs=vmem(),
        cost_estimate=cost(2),
        compiler_params=limit(8),
        name="place",
    )(x, kept, got).reshape(keep, v, j, k)


def solution(mesh):
    sizes = dict(mesh.shape)
    nx = sizes["gx"]
    chip = nx // 2

    def swap(array, step, axis="gx"):
        return lax.ppermute(array, axis, [(i, i ^ step) for i in range(sizes[axis])])

    def sum_columns(part, keep):
        for axis in ("gz", "gy"):
            step = 1
            while step < sizes[axis]:
                part = add(part, swap(part, step, axis), keep)
                step *= 2
        return part

    def everywhere(mine):
        far = swap(mine, chip)
        return [mine, swap(mine, 1), far, swap(far, 1)]

    def program(fields, var_scale, start_basis):
        v, rows, j, k = fields.shape
        rank = start_basis.shape[1]
        pad = -(-rows // LANE) * LANE
        me = lax.axis_index("gx").reshape(1)
        x = me // chip
        flat = fields.reshape(v, rows * j, k)
        (first,) = pack(flat, var_scale, x, rows, pad, j, False)
        *rest, ours = pack(flat, var_scale, x, rows, pad, j, True)
        theirs = [first, *rest]
        far = []
        for t in theirs:
            far.append(swap(t, chip))
        near_ours = swap(ours, 1)
        near_theirs = [swap(t, 1) for t in theirs]
        *halves, tall_high, tall_low, diag = diagonal(ours, theirs, near_ours, near_theirs, v)
        diag = sum_columns(diag, (*halves, tall_high, tall_low))
        diags = everywhere(diag)
        top = crossing(tall_high, tall_low, far[:2], None, 0)
        top = sum_columns(top, (*halves, tall_high, tall_low))
        bottom = crossing(tall_high, tall_low, far[2:3], None, 0)
        bottom = crossing(tall_high, tall_low, far[3:], bottom, far[2].shape[1])
        crosses = [everywhere(top), everywhere(sum_columns(bottom, halves))]
        both = [swap(f, 1) for f in far]
        start = start_basis.T.reshape(rank, nx, rows)
        start = jnp.pad(start, ((0, 0), (0, 0), (0, pad - rows))).reshape(rank, nx * pad)
        basis, kept, sent = solve(me, start, diags, crosses, *halves, far, both, nx, v)
        core = place(x, kept, swap(sent, chip), j)
        factor = basis[:, :, :rows].transpose(1, 0, 2).reshape(rank, nx * rows).T
        return factor, core

    in_specs = (P(None, "gx", "gy", "gz"), P(), P())
    out_specs = (P(), P("gx", None, "gy", "gz"))
    return jax.shard_map(program, mesh=mesh, in_specs=in_specs, out_specs=out_specs, check_vma=False)
```
